32 devices in a mesh: section: 4 (over y, x), ctx: 4 (over z), mp: 2 (over core).
Axes of the slice: x: 2, y: 2, z: 4, core: 2. Of those that a mesh axis runs over, the one named last changes fastest.
Arguments:
- head_input: bfloat16 [4, 1024, 2048], P('section', 'ctx', 'mp'), may hold values from -6 to 6
- state_proj: bfloat16 [4, 1024, 256], P('section', 'ctx'), may hold values from -6 to 6
- gate_input: bfloat16 [4, 1024, 2048], P('section', 'ctx', 'mp'), may hold values from -6 to 6
- step_raw: float32 [4, 32, 1024], P('section', 'mp', 'ctx'), may hold values from -2 to 2
- step_bias: float32 [4, 32], P('section', 'mp'), may hold values from -9.5 to -3
- decay_log: float32 [4, 32], P('section', 'mp'), may hold values from -7 to 1.5
- skip_gain: float32 [4, 32], P('section', 'mp'), may hold values from 0.5 to 1.5
- conv_head: float32 [4, 4, 2048], P('section', None, 'mp'), may hold values from -3 to 3
- conv_state: float32 [4, 4, 256], P('section'), may hold values from -3 to 3
- norm_gain: float32 [4, 2048], P('section', 'mp'), may hold values from 0.1 to 1.9
- next_weight: bfloat16 [4, 2048, 4096], P('section', 'ctx', 'mp'), may hold values from -0.125 to 0.125
Outputs:
- projected: bfloat16 [4, 1024, 4096], P('section', 'ctx', 'mp')
The draws below stay inside these ranges and needn't reach their ends.
All inputs are finite; a program needn't handle non-finite values.
Results may differ from the reference program's by a relative error of at most 0.0087.
Values may be sent and summed in bfloat16 or wider, within the bound.
A program may use at most 64 MiB of HBM per device.

```python
import jax
import jax.numpy as jnp
from jax import lax

HEADS = 32
HEAD_DIM = 64
STATE = 128
BLOCK = 256
CONV_TAPS = 4
MODEL_WIDTH = 4096
TOK_DEV = 256
FEATURES = 2048
LENGTH = 1024
SECTIONS = 4


def head_law(key):
    base = jax.random.fold_in(key, 29)
    flag_key, rate_key, size_key = jax.random.split(base, 3)
    fast_share = 0.5
    fast = jax.random.uniform(flag_key, (SECTIONS, HEADS), jnp.float32) < fast_share
    rate_unit = jax.random.uniform(rate_key, (SECTIONS, HEADS), jnp.float32)
    size_unit = jax.random.uniform(size_key, (SECTIONS, HEADS), jnp.float32)
    fast_rate = 0.02 * jnp.exp(rate_unit * jnp.log(2.0))
    slow_rate = 0.3 / LENGTH * jnp.exp(rate_unit * jnp.log(1.0 / 0.3))
    fast_size = 0.015 * jnp.exp(size_unit * jnp.log(0.04 / 0.015))
    slow_size = 0.5 / (7.0 * jnp.sqrt(1.0 * LENGTH)) * jnp.exp(size_unit * jnp.log(4.0))
    rate = jnp.where(fast, fast_rate, slow_rate)
    size = jnp.where(fast, fast_size, slow_size)
    return (rate, size)


def draw_decay_log(key, part):
    rate, size = head_law(key)
    return jnp.log(rate / size).astype(jnp.float32)


def draw_step_bias(key, part):
    rate, size = head_law(key)
    return jnp.log(jnp.expm1(size)).astype(jnp.float32)


def draw_step_raw(key, part):
    block_key, noise_key = jax.random.split(jax.random.fold_in(key, 31))
    block_total = LENGTH // TOK_DEV
    offsets = jax.random.uniform(block_key, (SECTIONS, HEADS, block_total), jnp.float32, minval=-0.7, maxval=0.7)
    noise = 0.4 * jax.random.truncated_normal(noise_key, -3.0, 3.0, (SECTIONS, HEADS, LENGTH), jnp.float32)
    return (noise + jnp.repeat(offsets, TOK_DEV, axis=2)).astype(jnp.float32)


def block_scale(key, dims, cuts, low, top_value):
    def one(dim, shards_of):
        heights = jax.random.uniform(jax.random.fold_in(jax.random.fold_in(key, 6), dim), (shards_of,), jnp.float32, low / len(cuts), top_value / len(cuts))
        return jnp.repeat(jnp.exp(heights), dims[dim] // shards_of).reshape((-1,) + (1,) * (len(dims) - dim - 1))

    loudness = one(*cuts[0])
    for cut in cuts[1:]:
        loudness = loudness * one(*cut)
    return loudness


def scatter_about(key, shape, width, limit, cuts=(), kind=jnp.bfloat16):
    entries = jax.random.normal(key, shape, jnp.float32) * width
    if len(cuts) > 0:
        entries = block_scale(key, shape, cuts, -0.22, 0.18) * entries
    return jnp.clip(entries, min=-limit, max=limit).astype(kind)


def setup_inputs(seed: int = 0) -> dict:
    key_of = jax.random.split(jax.random.key(seed), 12)
    head_input = scatter_about(key_of[0], (SECTIONS, LENGTH, FEATURES), 1.0, 6.0, ((0, 4), (1, 4), (2, 2)))
    state_proj = scatter_about(key_of[1], (SECTIONS, LENGTH, 2 * STATE), 1.0, 6.0, ((0, 4), (1, 4)))
    gate_input = scatter_about(key_of[2], (SECTIONS, LENGTH, FEATURES), 1.0, 6.0, ((0, 4), (1, 4), (2, 2)))
    step_raw = draw_step_raw(jax.random.fold_in(key_of[11], 71), 0)
    step_bias = draw_step_bias(jax.random.fold_in(key_of[11], 71), 0)
    decay_log = draw_decay_log(jax.random.fold_in(key_of[11], 71), 0)
    skip_gain = jnp.clip(0.5 + 1.0 * jax.random.uniform(key_of[6], (SECTIONS, HEADS), jnp.float32) ** block_scale(key_of[6], (SECTIONS, HEADS), ((0, 4), (1, 2)), -0.2, 0.2), 0.5, 1.5)
    conv_head = scatter_about(key_of[7], (SECTIONS, CONV_TAPS, FEATURES), CONV_TAPS ** -0.5, 3.0, ((0, 4), (2, 2)), jnp.float32)
    conv_state = scatter_about(key_of[8], (SECTIONS, CONV_TAPS, 2 * STATE), CONV_TAPS ** -0.5, 3.0, ((0, 4),), jnp.float32)
    norm_gain = jnp.clip(1.0 + 0.18 * jax.random.normal(key_of[9], (SECTIONS, FEATURES), jnp.float32), 0.1, 1.9)
    next_weight = scatter_about(key_of[10], (SECTIONS, FEATURES, MODEL_WIDTH), FEATURES ** -0.5, 0.125, ((0, 4), (1, 4), (2, 2)))
    return dict(head_input=head_input, state_proj=state_proj, gate_input=gate_input, step_raw=step_raw, step_bias=step_bias, decay_log=decay_log, skip_gain=skip_gain, conv_head=conv_head, conv_state=conv_state, norm_gain=norm_gain, next_weight=next_weight)


NORM_FLOOR = 0.25
HIGHEST = lax.Precision.HIGHEST

def causal_conv(sequence, weights):
    length = sequence.shape[0]
    padding = jnp.zeros((weights.shape[0] - 1, sequence.shape[1]), sequence.dtype)
    padded = jnp.concatenate([padding, sequence], axis=0).astype(jnp.float32)
    summed = jnp.zeros(sequence.shape, jnp.float32)
    for offset in range(weights.shape[0]):
        summed = summed + weights[offset] * padded[offset:offset + length]
    return summed

def mixer(head_input, state_proj, gate_input, step_raw, step_bias, decay_log, skip_gain, conv_head, conv_state, norm_gain):
    conv_x = jax.nn.silu(causal_conv(head_input, conv_head)).astype(jnp.bfloat16)
    conv_bc = causal_conv(state_proj, conv_state).astype(jnp.bfloat16)
    block_count = LENGTH // BLOCK
    blocks_x = conv_x.reshape(block_count, BLOCK, HEADS, HEAD_DIM)
    blocks_b = conv_bc[:, :STATE].reshape(block_count, BLOCK, STATE)
    blocks_c = conv_bc[:, STATE:].reshape(block_count, BLOCK, STATE)
    step_size = jax.nn.softplus(step_raw + step_bias[:, None])
    log_decay = -jnp.exp(decay_log)[:, None] * step_size
    blocks_step = step_size.reshape(HEADS, block_count, BLOCK).transpose(1, 0, 2)
    blocks_decay = log_decay.reshape(HEADS, block_count, BLOCK).transpose(1, 0, 2)
    row_index = lax.broadcasted_iota(jnp.int32, (BLOCK, BLOCK), 0)
    col_index = lax.broadcasted_iota(jnp.int32, (BLOCK, BLOCK), 1)
    causal_mask = row_index >= col_index

    def block_step(carried, block_items):
        part_x, part_b, part_c, part_step, part_decay = block_items
        cumulative = jnp.cumsum(part_decay, axis=1)
        scores = jnp.dot(part_c, part_b.T, preferred_element_type=jnp.float32)
        decay_diff = jnp.where(causal_mask, cumulative[:, :, None] - cumulative[:, None, :], 0.0)
        mix_weight = jnp.where(causal_mask, scores[None] * jnp.exp(decay_diff) * part_step[:, None, :], 0.0).astype(jnp.bfloat16)
        intra_part = jnp.einsum('hts,shp->thp', mix_weight.astype(jnp.float32), part_x.astype(jnp.float32), precision=HIGHEST)
        tail_weight = jnp.exp(cumulative[:, -1:] - cumulative) * part_step
        weighted_b = (part_b.astype(jnp.float32)[None] * tail_weight[:, :, None]).astype(jnp.bfloat16)
        update = jnp.einsum('shp,hsn->hpn', part_x.astype(jnp.float32), weighted_b.astype(jnp.float32), precision=HIGHEST)
        inter_part = jnp.einsum('tn,hpn->thp', part_c.astype(jnp.float32), carried, precision=HIGHEST) * jnp.exp(cumulative).T[:, :, None]
        output = intra_part + inter_part + skip_gain[None, :, None] * part_x.astype(jnp.float32)
        next_carried = jnp.exp(cumulative[:, -1])[:, None, None] * carried + update
        return (next_carried, output)
    start_state = jnp.zeros((HEADS, HEAD_DIM, STATE), jnp.float32)
    last_state, outputs = lax.scan(block_step, start_state, (blocks_x, blocks_b, blocks_c, blocks_step, blocks_decay))
    mixer_y = outputs.reshape(LENGTH, FEATURES)
    gated = mixer_y * jax.nn.silu(gate_input.astype(jnp.float32))
    mean_square = lax.optimization_barrier(jnp.sum(gated * gated, axis=1)) / FEATURES
    return (gated * lax.rsqrt(mean_square + NORM_FLOOR)[:, None] * norm_gain[None]).astype(jnp.bfloat16)

def reference(head_input, state_proj, gate_input, step_raw, step_bias, decay_log, skip_gain, conv_head, conv_state, norm_gain, next_weight):
    normed_all = []
    for section_index in range(SECTIONS):
        normed_all.append(mixer(head_input[section_index], state_proj[section_index], gate_input[section_index], step_raw[section_index], step_bias[section_index], decay_log[section_index], skip_gain[section_index], conv_head[section_index], conv_state[section_index], norm_gain[section_index]))
    projected = []
    for section_index in range(SECTIONS):
        source = normed_all[(section_index - 1) % SECTIONS]
        projected.append(jnp.dot(source, next_weight[section_index], preferred_element_type=jnp.float32).astype(jnp.bfloat16))
    return jnp.stack(projected)
```

```python
import jax
import jax.numpy as jnp
from jax import lax
from jax.sharding import PartitionSpec as P

STATE = 128
BLOCK = 256
FEATURES = 2048


NORM_FLOOR = 0.25
FEW = 8
HIGHEST = lax.Precision.HIGHEST


def from_behind(value, axis, steps):
    count = lax.axis_size(axis)
    first, last = (max(0, -steps), min(count, count - steps))
    return lax.ppermute(value, axis, [(source, source + steps) for source in range(first, last)])


def chain(total, update, axis):
    count = lax.axis_size(axis)
    place = lax.axis_index(axis)
    decay = jnp.exp(total)[:, None, None]
    state = jnp.zeros_like(update)

    def passed(state):
        return (decay * state + update).astype(jnp.bfloat16)

    if count > FEW:
        pairs = [(source, source + 1) for source in range(count - 1)]
        return lax.fori_loop(
            1,
            count,
            lambda _, state: lax.ppermute(passed(state), axis, pairs).astype(jnp.float32),
            state,
        )
    for step in range(1, count):
        came = lax.ppermute(passed(state), axis, [(step - 1, step)])
        state = jnp.where(place == step, came.astype(jnp.float32), state)
    return state


def gather_half(rows):
    count = lax.axis_size("ctx")
    half = count // 2
    if count > FEW:
        groups = [list(range(base, base + half)) for base in (0, half)]
        return [lax.all_gather(rows, "ctx", axis_index_groups=groups, tiled=True)]
    blocks = [rows]
    for step in range(1, half):
        pairs = [
            (base + (place + step) % half, base + place)
            for base in (0, half)
            for place in range(half)
        ]
        blocks.append(lax.ppermute(rows, "ctx", pairs))
    return blocks


def route(value):
    sections, count, cores = (lax.axis_size(a) for a in ("section", "ctx", "mp"))
    half = count // 2
    pairs = []
    for section in range(sections):
        for place in range(count):
            for core in range(cores):
                source = (section * count + place) * cores + core
                target_place = place % half + half * core
                target = (((section + 1) % sections) * count + target_place) * cores
                pairs.append((source, target + place // half))
    return lax.ppermute(value, ("section", "ctx", "mp"), pairs)


def project(normed):
    count = lax.axis_size("ctx")
    half = count // 2
    place = lax.axis_index("ctx")
    side = place // half
    arrived = route(normed)
    other = lax.ppermute(arrived, "mp", [(0, 1), (1, 0)])
    mine = lax.axis_index("mp") == side
    own = jnp.where(mine, arrived, other)
    mirror = jnp.where(mine, other, arrived)
    return own, mirror


def causal_conv(sequence, previous, weights):
    length = sequence.shape[0]
    padded = jnp.concatenate([previous, sequence], axis=0).astype(jnp.float32)
    summed = jnp.zeros(sequence.shape, jnp.float32)
    for offset in range(weights.shape[0]):
        summed = summed + weights[offset] * padded[offset : offset + length]
    return summed


def shards(
    head_input,
    state_proj,
    gate_input,
    step_raw,
    step_bias,
    decay_log,
    skip_gain,
    conv_head,
    conv_state,
    norm_gain,
    next_weight,
):
    tap_count = conv_head.shape[1]
    token_count = head_input.shape[1]
    local_width = head_input.shape[2]
    head_count = step_raw.shape[1]
    head_width = local_width // head_count
    block_count = token_count // BLOCK
    parts = 4
    early = 3
    piece = next_weight.shape[2] // parts
    weight_parts = [
        gather_half(next_weight[0, :, part * piece : (part + 1) * piece])
        for part in range(parts)
    ]
    tails = jnp.concatenate(
        [
            head_input[0, token_count - tap_count + 1 :],
            state_proj[0, token_count - tap_count + 1 :],
        ],
        axis=1,
    )
    previous = from_behind(tails, "ctx", 1)
    conv_x = jax.nn.silu(
        causal_conv(head_input[0], previous[:, :local_width], conv_head[0])
    ).astype(jnp.bfloat16)
    conv_bc = causal_conv(state_proj[0], previous[:, local_width:], conv_state[0]).astype(
        jnp.bfloat16
    )
    blocks_x = conv_x.reshape(block_count, BLOCK, head_count, head_width)
    blocks_b = conv_bc[:, :STATE].reshape(block_count, BLOCK, STATE)
    blocks_c = conv_bc[:, STATE:].reshape(block_count, BLOCK, STATE)
    step_size = jax.nn.softplus(step_raw[0] + step_bias[0][:, None])
    log_decay = -jnp.exp(decay_log[0])[:, None] * step_size
    blocks_step = step_size.reshape(head_count, block_count, BLOCK)
    blocks_decay = log_decay.reshape(head_count, block_count, BLOCK)
    row_index = lax.broadcasted_iota(jnp.int32, (BLOCK, BLOCK), 0)
    col_index = lax.broadcasted_iota(jnp.int32, (BLOCK, BLOCK), 1)
    causal_mask = row_index >= col_index
    lower_tri = causal_mask.astype(jnp.float32)
    cumulative = jnp.einsum("hcs,ts->hct", blocks_decay, lower_tri, precision=HIGHEST)
    scores = jnp.einsum("ctn,csn->cts", blocks_c, blocks_b, preferred_element_type=jnp.float32)
    decay_diff = jnp.where(causal_mask, cumulative[..., :, None] - cumulative[..., None, :], 0.0)
    mix_weight = jnp.where(
        causal_mask, scores[None] * jnp.exp(decay_diff) * blocks_step[:, :, None, :], 0.0
    ).astype(jnp.bfloat16)
    intra_part = jnp.einsum(
        "hcts,cshp->cthp", mix_weight, blocks_x, preferred_element_type=jnp.float32
    )
    tail_weight = jnp.exp(cumulative[..., -1:] - cumulative) * blocks_step
    weighted_b = (blocks_b.astype(jnp.float32)[None] * tail_weight[..., None]).astype(jnp.bfloat16)
    updates = jnp.einsum(
        "cshp,hcsn->chpn", blocks_x, weighted_b, preferred_element_type=jnp.float32
    )
    totals = cumulative[..., -1]
    full_states = chain(totals[:, 0], updates[0], "ctx")[None]
    inter_part = (
        jnp.einsum("ctn,chpn->cthp", blocks_c.astype(jnp.float32), full_states, precision=HIGHEST)
        * jnp.exp(cumulative).transpose(1, 2, 0)[..., None]
    )
    output = (
        intra_part + inter_part + skip_gain[0][None, None, :, None] * blocks_x.astype(jnp.float32)
    )
    gated = output.reshape(token_count, local_width) * jax.nn.silu(
        gate_input[0].astype(jnp.float32)
    )
    squares = lax.psum(jnp.sum(gated * gated, axis=1), "mp")
    mean_square = squares / FEATURES
    normed = (gated * lax.rsqrt(mean_square + NORM_FLOOR)[:, None] * norm_gain[0][None]).astype(
        jnp.bfloat16
    )
    normed, weight_parts[:early] = lax.optimization_barrier((normed, weight_parts[:early]))
    own, mirror = project(normed)
    count = lax.axis_size("ctx")
    half = count // 2
    place = lax.axis_index("ctx")
    depth = next_weight.shape[1]
    opposite = [(source, (source + half) % count) for source in range(count)]

    def product(rows, blocks):
        total = None
        for step, block in enumerate(blocks):
            start = (place + step) % half * depth if len(blocks) > 1 else 0
            term = jnp.dot(
                lax.dynamic_slice_in_dim(rows, start, block.shape[0], 1),
                block,
                preferred_element_type=jnp.float32,
            )
            total = term if total is None else total + term
        return total

    results = []
    for blocks in weight_parts:
        sent = product(mirror, blocks).astype(jnp.bfloat16)
        came = lax.ppermute(sent, "ctx", opposite)
        results.append((product(own, blocks) + came.astype(jnp.float32)).astype(jnp.bfloat16))
    return jnp.concatenate(results, axis=1)[None]


def solution(mesh):
    return jax.shard_map(
        shards,
        mesh=mesh,
        in_specs=(
            P("section", "ctx", "mp"),
            P("section", "ctx", None),
            P("section", "ctx", "mp"),
            P("section", "mp", "ctx"),
            P("section", "mp"),
            P("section", "mp"),
            P("section", "mp"),
            P("section", None, "mp"),
            P("section", None, None),
            P("section", "mp"),
            P("section", "ctx", "mp"),
        ),
        out_specs=P("section", "ctx", "mp"),
        check_vma=False,
    )
```

```python
import functools

import jax
import jax.numpy as jnp
from jax import lax
from jax.experimental import pallas as pl
from jax.experimental.pallas import tpu as pltpu
from jax.sharding import PartitionSpec as P

STATE = 128
BLOCK = 256
FEATURES = 2048


NORM_FLOOR = 0.25
FEW = 8
HIGHEST = lax.Precision.HIGHEST


def from_behind(value, axis, steps):
    count = lax.axis_size(axis)
    first, last = (max(0, -steps), min(count, count - steps))
    return lax.ppermute(value, axis, [(source, source + steps) for source in range(first, last)])


def chain(total, update, axis):
    count = lax.axis_size(axis)
    place = lax.axis_index(axis)
    decay = jnp.exp(total)[:, None, None]
    state = jnp.zeros_like(update)

    def passed(state):
        return (decay * state + update).astype(jnp.bfloat16)

    if count > FEW:
        pairs = [(source, source + 1) for source in range(count - 1)]
        return lax.fori_loop(
            1,
            count,
            lambda _, state: lax.ppermute(passed(state), axis, pairs).astype(jnp.float32),
            state,
        )
    for step in range(1, count):
        came = lax.ppermute(passed(state), axis, [(step - 1, step)])
        state = jnp.where(place == step, came.astype(jnp.float32), state)
    return state


def gather_half(rows):
    count = lax.axis_size("ctx")
    half = count // 2
    groups = [list(range(base, base + half)) for base in (0, half)]
    return lax.all_gather(rows, "ctx", axis_index_groups=groups, tiled=True)


def project_kernel(
    sections,
    count,
    chunks,
    normed,
    weight,
    out,
    held,
    blocks,
    sends,
    recvs,
    weight_sem,
    route_send,
    route_recv,
    pass_send,
    pass_recv,
    part_send,
    part_recv,
):
    section, place, core = (lax.axis_index(a) for a in ("section", "ctx", "mp"))
    half = count // 2
    side = place // half
    rows = normed.shape[0] // 2
    width = out.shape[1] // chunks
    load = pltpu.make_async_copy(weight, held, weight_sem)
    load.start()

    def at(section, place, core):
        return {"section": section, "ctx": place, "mp": core}

    after = lax.rem(section + 1, sections)
    before = lax.rem(section + sections - 1, sections)
    mirror = lax.rem(place + half, count)
    target = lax.rem(place, half) + half * core
    peer = at(section, place, 1 - core)
    opposite = at(section, mirror, core)
    barrier = pltpu.get_barrier_semaphore()
    friends = [
        at(after, target, 0),
        at(after, target, 1),
        at(before, place, side),
        at(before, mirror, side),
        peer,
        opposite,
    ]
    for friend in friends:
        pl.semaphore_signal(
            barrier, inc=1, device_id=friend, device_id_type=pl.DeviceIdType.MESH
        )
    pl.semaphore_wait(barrier, len(friends))

    slot = lax.rem(side + core, 2)
    routes = []
    for to in range(2):
        piece = pl.ds(to * rows, rows)
        routes.append(
            pltpu.make_async_remote_copy(
                src_ref=normed.at[piece],
                dst_ref=blocks.at[slot, piece],
                send_sem=route_send.at[to],
                recv_sem=route_recv.at[slot],
                device_id=at(after, target, to),
                device_id_type=pl.DeviceIdType.MESH,
            )
        )
        routes[-1].start()
    mine = pl.ds(pl.multiple_of(core * rows, rows), rows)
    passes = []
    for which in (1, 0):
        landed = blocks.at[which, mine]
        pltpu.make_async_copy(landed, landed, route_recv.at[which]).wait()
        passes.append(
            pltpu.make_async_remote_copy(
                src_ref=landed,
                dst_ref=landed,
                send_sem=pass_send.at[which],
                recv_sem=pass_recv.at[which],
                device_id=peer,
                device_id_type=pl.DeviceIdType.MESH,
            )
        )
        passes[-1].start()

    def part(index):
        return pltpu.make_async_remote_copy(
            src_ref=sends.at[index],
            dst_ref=recvs.at[index],
            send_sem=part_send.at[index],
            recv_sem=part_recv.at[index],
            device_id=opposite,
            device_id_type=pl.DeviceIdType.MESH,
        )

    def product(which, index):
        columns = pl.ds(pl.multiple_of(index * width, width), width)
        return jnp.dot(blocks[which], held[:, columns], preferred_element_type=jnp.float32)

    load.wait()
    passes[0].wait_recv()

    def give(index, carry):
        sends[index] = product(1, index).astype(sends.dtype)

        @pl.when(index > 0)
        def _():
            part(index - 1).start()

        return carry

    lax.fori_loop(0, chunks, give, 0)
    passes[1].wait_recv()
    part(chunks - 1).start()

    def take(index, carry):
        own = product(0, index)
        part(index).wait_recv()
        columns = pl.ds(pl.multiple_of(index * width, width), width)
        out[:, columns] = (own + recvs[index].astype(jnp.float32)).astype(out.dtype)
        part(index).wait_send()
        return carry

    lax.fori_loop(0, chunks, take, 0)
    for copy in routes + passes:
        copy.wait_send()


def project(normed, weight):
    sections, count = (lax.axis_size(a) for a in ("section", "ctx"))
    rows, depth = normed.shape
    width = weight.shape[1]
    chunks = 8
    piece = (chunks, rows, width // chunks)
    return pl.pallas_call(
        functools.partial(project_kernel, sections, count, chunks),
        out_shape=jax.ShapeDtypeStruct((rows, width), jnp.bfloat16),
        in_specs=[
            pl.BlockSpec(memory_space=pltpu.VMEM),
            pl.BlockSpec(memory_space=pl.ANY),
        ],
        out_specs=pl.BlockSpec(memory_space=pltpu.VMEM),
        scratch_shapes=[
            pltpu.VMEM(weight.shape, jnp.bfloat16),
            pltpu.VMEM((2, rows, depth), jnp.bfloat16),
            pltpu.VMEM(piece, jnp.bfloat16),
            pltpu.VMEM(piece, jnp.bfloat16),
            pltpu.SemaphoreType.DMA,
            pltpu.SemaphoreType.DMA((2,)),
            pltpu.SemaphoreType.DMA((2,)),
            pltpu.SemaphoreType.DMA((2,)),
            pltpu.SemaphoreType.DMA((2,)),
            pltpu.SemaphoreType.DMA((chunks,)),
            pltpu.SemaphoreType.DMA((chunks,)),
        ],
        cost_estimate=pl.CostEstimate(
            flops=4 * rows * depth * width, bytes_accessed=2 * depth * width, transcendentals=0
        ),
        compiler_params=pltpu.CompilerParams(collective_id=0, has_side_effects=True),
        name="project",
    )(normed, weight)


def causal_conv(sequence, previous, weights):
    length = sequence.shape[0]
    padded = jnp.concatenate([previous, sequence], axis=0).astype(jnp.float32)
    summed = jnp.zeros(sequence.shape, jnp.float32)
    for offset in range(weights.shape[0]):
        summed = summed + weights[offset] * padded[offset : offset + length]
    return summed


def shards(
    head_input,
    state_proj,
    gate_input,
    step_raw,
    step_bias,
    decay_log,
    skip_gain,
    conv_head,
    conv_state,
    norm_gain,
    next_weight,
):
    tap_count = conv_head.shape[1]
    token_count = head_input.shape[1]
    local_width = head_input.shape[2]
    head_count = step_raw.shape[1]
    head_width = local_width // head_count
    block_count = token_count // BLOCK
    gathered_weight = gather_half(next_weight[0])
    tails = jnp.concatenate(
        [
            head_input[0, token_count - tap_count + 1 :],
            state_proj[0, token_count - tap_count + 1 :],
        ],
        axis=1,
    )
    previous = from_behind(tails, "ctx", 1)
    conv_x = jax.nn.silu(
        causal_conv(head_input[0], previous[:, :local_width], conv_head[0])
    ).astype(jnp.bfloat16)
    conv_bc = causal_conv(state_proj[0], previous[:, local_width:], conv_state[0]).astype(
        jnp.bfloat16
    )
    blocks_x = conv_x.reshape(block_count, BLOCK, head_count, head_width)
    blocks_b = conv_bc[:, :STATE].reshape(block_count, BLOCK, STATE)
    blocks_c = conv_bc[:, STATE:].reshape(block_count, BLOCK, STATE)
    step_size = jax.nn.softplus(step_raw[0] + step_bias[0][:, None])
    log_decay = -jnp.exp(decay_log[0])[:, None] * step_size
    blocks_step = step_size.reshape(head_count, block_count, BLOCK)
    blocks_decay = log_decay.reshape(head_count, block_count, BLOCK)
    row_index = lax.broadcasted_iota(jnp.int32, (BLOCK, BLOCK), 0)
    col_index = lax.broadcasted_iota(jnp.int32, (BLOCK, BLOCK), 1)
    causal_mask = row_index >= col_index
    lower_tri = causal_mask.astype(jnp.float32)
    cumulative = jnp.einsum("hcs,ts->hct", blocks_decay, lower_tri, precision=HIGHEST)
    scores = jnp.einsum("ctn,csn->cts", blocks_c, blocks_b, preferred_element_type=jnp.float32)
    decay_diff = jnp.where(causal_mask, cumulative[..., :, None] - cumulative[..., None, :], 0.0)
    mix_weight = jnp.where(
        causal_mask, scores[None] * jnp.exp(decay_diff) * blocks_step[:, :, None, :], 0.0
    ).astype(jnp.bfloat16)
    intra_part = jnp.einsum(
        "hcts,cshp->cthp", mix_weight, blocks_x, preferred_element_type=jnp.float32
    )
    tail_weight = jnp.exp(cumulative[..., -1:] - cumulative) * blocks_step
    weighted_b = (blocks_b.astype(jnp.float32)[None] * tail_weight[..., None]).astype(jnp.bfloat16)
    updates = jnp.einsum(
        "cshp,hcsn->chpn", blocks_x, weighted_b, preferred_element_type=jnp.float32
    )
    totals = cumulative[..., -1]
    full_states = chain(totals[:, 0], updates[0], "ctx")[None]
    inter_part = (
        jnp.einsum("ctn,chpn->cthp", blocks_c.astype(jnp.float32), full_states, precision=HIGHEST)
        * jnp.exp(cumulative).transpose(1, 2, 0)[..., None]
    )
    output = (
        intra_part + inter_part + skip_gain[0][None, None, :, None] * blocks_x.astype(jnp.float32)
    )
    gated = output.reshape(token_count, local_width) * jax.nn.silu(
        gate_input[0].astype(jnp.float32)
    )
    squares = lax.psum(jnp.sum(gated * gated, axis=1), "mp")
    mean_square = squares / FEATURES
    normed = (gated * lax.rsqrt(mean_square + NORM_FLOOR)[:, None] * norm_gain[0][None]).astype(
        jnp.bfloat16
    )
    return project(normed, gathered_weight)[None]


def solution(mesh):
    return jax.shard_map(
        shards,
        mesh=mesh,
        in_specs=(
            P("section", "ctx", "mp"),
            P("section", "ctx", None),
            P("section", "ctx", "mp"),
            P("section", "mp", "ctx"),
            P("section", "mp"),
            P("section", "mp"),
            P("section", "mp"),
            P("section", None, "mp"),
            P("section", None, None),
            P("section", "mp"),
            P("section", "ctx", "mp"),
        ),
        out_specs=P("section", "ctx", "mp"),
        check_vma=False,
    )
```

```python
import functools

import jax
import jax.numpy as jnp
from jax import lax
from jax.experimental import pallas as pl
from jax.experimental.pallas import tpu as pltpu
from jax.sharding import PartitionSpec as P

STATE = 128
BLOCK = 256
FEATURES = 2048


NORM_FLOOR = 0.25
FEW = 8
HIGHEST = lax.Precision.HIGHEST


def from_behind(value, axis, steps):
    count = lax.axis_size(axis)
    first, last = (max(0, -steps), min(count, count - steps))
    return lax.ppermute(value, axis, [(source, source + steps) for source in range(first, last)])


def chain(total, update, axis):
    count = lax.axis_size(axis)
    place = lax.axis_index(axis)
    decay = jnp.exp(total)[:, None, None]
    state = jnp.zeros_like(update)

    def passed(state):
        return (decay * state + update).astype(jnp.bfloat16)

    if count > FEW:
        pairs = [(source, source + 1) for source in range(count - 1)]
        return lax.fori_loop(
            1,
            count,
            lambda _, state: lax.ppermute(passed(state), axis, pairs).astype(jnp.float32),
            state,
        )
    for step in range(1, count):
        came = lax.ppermute(passed(state), axis, [(step - 1, step)])
        state = jnp.where(place == step, came.astype(jnp.float32), state)
    return state


def gather_half(rows):
    count = lax.axis_size("ctx")
    half = count // 2
    blocks = []
    for step in range(1, half):
        pairs = [
            (base + (place + step) % half, base + place)
            for base in (0, half)
            for place in range(half)
        ]
        blocks.append(lax.ppermute(rows, "ctx", pairs))
    return jnp.concatenate(blocks, axis=0) if len(blocks) > 1 else blocks[0]


def project_kernel(
    sections,
    count,
    chunks,
    early,
    normed,
    weight,
    gathered,
    out,
    held,
    blocks,
    sends,
    recvs,
    weight_sem,
    route_send,
    route_recv,
    pass_send,
    pass_recv,
    part_send,
    part_recv,
    late_send,
    late_recv,
):
    section, place, core = (lax.axis_index(a) for a in ("section", "ctx", "mp"))
    half = count // 2
    side = place // half
    rows = normed.shape[0] // 2
    width = out.shape[1] // chunks
    depth = weight.shape[0]
    inner = lax.rem(place, half)

    def rows_of(owner):
        return pl.ds(pl.multiple_of(owner * depth, depth), depth)

    loads = [pltpu.make_async_copy(weight, held.at[rows_of(inner)], weight_sem.at[0])]
    for step in range(1, half):
        loads.append(
            pltpu.make_async_copy(
                gathered.at[pl.ds((step - 1) * depth, depth)],
                held.at[rows_of(lax.rem(inner + step, half)), pl.ds(0, early * width)],
                weight_sem.at[step],
            )
        )
    for load in loads:
        load.start()

    def at(section, place, core):
        return {"section": section, "ctx": place, "mp": core}

    after = lax.rem(section + 1, sections)
    before = lax.rem(section + sections - 1, sections)
    mirror = lax.rem(place + half, count)
    target = lax.rem(place, half) + half * core
    peer = at(section, place, 1 - core)
    opposite = at(section, mirror, core)
    barrier = pltpu.get_barrier_semaphore()
    friends = [
        at(after, target, 0),
        at(after, target, 1),
        at(before, place, side),
        at(before, mirror, side),
        peer,
        opposite,
    ]
    siblings = [
        at(section, side * half + lax.rem(inner + step, half), core) for step in range(1, half)
    ]
    friends += siblings
    for friend in friends:
        pl.semaphore_signal(
            barrier, inc=1, device_id=friend, device_id_type=pl.DeviceIdType.MESH
        )
    pl.semaphore_wait(barrier, len(friends))

    slot = lax.rem(side + core, 2)
    routes = []
    for to in range(2):
        piece = pl.ds(to * rows, rows)
        routes.append(
            pltpu.make_async_remote_copy(
                src_ref=normed.at[piece],
                dst_ref=blocks.at[slot, piece],
                send_sem=route_send.at[to],
                recv_sem=route_recv.at[slot],
                device_id=at(after, target, to),
                device_id_type=pl.DeviceIdType.MESH,
            )
        )
        routes[-1].start()

    def late(step, index):
        columns = pl.ds(pl.multiple_of(index * width, width), width)
        return pltpu.make_async_remote_copy(
            src_ref=weight.at[:, columns],
            dst_ref=held.at[rows_of(inner), columns],
            send_sem=late_send.at[step - 1, index - early],
            recv_sem=late_recv.at[step - 1, index - early],
            device_id=siblings[step - 1],
            device_id_type=pl.DeviceIdType.MESH,
        )

    for index in range(early, chunks):
        for step in range(1, half):
            late(step, index).start()
    mine = pl.ds(pl.multiple_of(core * rows, rows), rows)
    passes = []
    for which in (1, 0):
        landed = blocks.at[which, mine]
        pltpu.make_async_copy(landed, landed, route_recv.at[which]).wait()
        passes.append(
            pltpu.make_async_remote_copy(
                src_ref=landed,
                dst_ref=landed,
                send_sem=pass_send.at[which],
                recv_sem=pass_recv.at[which],
                device_id=peer,
                device_id_type=pl.DeviceIdType.MESH,
            )
        )
        passes[-1].start()

    def part(index):
        return pltpu.make_async_remote_copy(
            src_ref=sends.at[index],
            dst_ref=recvs.at[index],
            send_sem=part_send.at[index],
            recv_sem=part_recv.at[index],
            device_id=opposite,
            device_id_type=pl.DeviceIdType.MESH,
        )

    def product(which, index):
        columns = pl.ds(pl.multiple_of(index * width, width), width)
        return jnp.dot(blocks[which], held[:, columns], preferred_element_type=jnp.float32)

    for load in loads:
        load.wait()
    passes[0].wait_recv()

    def give(index, carry):
        sends[index] = product(1, index).astype(sends.dtype)

        @pl.when(index > 0)
        def _():
            part(index - 1).start()

        return carry

    lax.fori_loop(0, early, give, 0)

    def give_late(index, carry):
        columns = pl.ds(pl.multiple_of(index * width, width), width)
        for step in range(1, half):
            source = lax.rem(inner + half - step, half)
            landed = held.at[rows_of(source), columns]
            pltpu.make_async_copy(landed, landed, late_recv.at[step - 1, index - early]).wait()
        return give(index, carry)

    lax.fori_loop(early, chunks, give_late, 0)
    passes[1].wait_recv()
    part(chunks - 1).start()

    def take(index, carry):
        own = product(0, index)
        part(index).wait_recv()
        columns = pl.ds(pl.multiple_of(index * width, width), width)
        out[:, columns] = (own + recvs[index].astype(jnp.float32)).astype(out.dtype)
        part(index).wait_send()
        return carry

    lax.fori_loop(0, chunks, take, 0)
    for copy in routes + passes:
        copy.wait_send()
    for index in range(early, chunks):
        for step in range(1, half):
            late(step, index).wait_send()


CHUNKS = 8
EARLY = 4


def project(normed, weight, gathered):
    sections, count = (lax.axis_size(a) for a in ("section", "ctx"))
    rows, depth = normed.shape
    width = weight.shape[1]
    half = count // 2
    chunks, early = CHUNKS, EARLY
    piece = (chunks, rows, width // chunks)
    return pl.pallas_call(
        functools.partial(project_kernel, sections, count, chunks, early),
        out_shape=jax.ShapeDtypeStruct((rows, width), jnp.bfloat16),
        in_specs=[
            pl.BlockSpec(memory_space=pltpu.VMEM),
            pl.BlockSpec(memory_space=pl.ANY),
            pl.BlockSpec(memory_space=pl.ANY),
        ],
        out_specs=pl.BlockSpec(memory_space=pltpu.VMEM),
        scratch_shapes=[
            pltpu.VMEM((depth, width), jnp.bfloat16),
            pltpu.VMEM((2, rows, depth), jnp.bfloat16),
            pltpu.VMEM(piece, jnp.bfloat16),
            pltpu.VMEM(piece, jnp.bfloat16),
            pltpu.SemaphoreType.DMA((half,)),
            pltpu.SemaphoreType.DMA((2,)),
            pltpu.SemaphoreType.DMA((2,)),
            pltpu.SemaphoreType.DMA((2,)),
            pltpu.SemaphoreType.DMA((2,)),
            pltpu.SemaphoreType.DMA((chunks,)),
            pltpu.SemaphoreType.DMA((chunks,)),
            pltpu.SemaphoreType.DMA((half - 1, chunks - early)),
            pltpu.SemaphoreType.DMA((half - 1, chunks - early)),
        ],
        cost_estimate=pl.CostEstimate(
            flops=4 * rows * depth * width, bytes_accessed=2 * depth * width, transcendentals=0
        ),
        compiler_params=pltpu.CompilerParams(collective_id=0, has_side_effects=True),
        name="project",
    )(normed, weight, gathered)


def causal_conv(sequence, previous, weights):
    length = sequence.shape[0]
    padded = jnp.concatenate([previous, sequence], axis=0).astype(jnp.float32)
    summed = jnp.zeros(sequence.shape, jnp.float32)
    for offset in range(weights.shape[0]):
        summed = summed + weights[offset] * padded[offset : offset + length]
    return summed


def shards(
    head_input,
    state_proj,
    gate_input,
    step_raw,
    step_bias,
    decay_log,
    skip_gain,
    conv_head,
    conv_state,
    norm_gain,
    next_weight,
):
    tap_count = conv_head.shape[1]
    token_count = head_input.shape[1]
    local_width = head_input.shape[2]
    head_count = step_raw.shape[1]
    head_width = local_width // head_count
    block_count = token_count // BLOCK
    early_columns = next_weight.shape[2] // CHUNKS * EARLY
    gathered = gather_half(next_weight[0, :, :early_columns])
    tails = jnp.concatenate(
        [
            head_input[0, token_count - tap_count + 1 :],
            state_proj[0, token_count - tap_count + 1 :],
        ],
        axis=1,
    )
    previous = from_behind(tails, "ctx", 1)
    conv_x = jax.nn.silu(
        causal_conv(head_input[0], previous[:, :local_width], conv_head[0])
    ).astype(jnp.bfloat16)
    conv_bc = causal_conv(state_proj[0], previous[:, local_width:], conv_state[0]).astype(
        jnp.bfloat16
    )
    blocks_x = conv_x.reshape(block_count, BLOCK, head_count, head_width)
    blocks_b = conv_bc[:, :STATE].reshape(block_count, BLOCK, STATE)
    blocks_c = conv_bc[:, STATE:].reshape(block_count, BLOCK, STATE)
    step_size = jax.nn.softplus(step_raw[0] + step_bias[0][:, None])
    log_decay = -jnp.exp(decay_log[0])[:, None] * step_size
    blocks_step = step_size.reshape(head_count, block_count, BLOCK)
    blocks_decay = log_decay.reshape(head_count, block_count, BLOCK)
    row_index = lax.broadcasted_iota(jnp.int32, (BLOCK, BLOCK), 0)
    col_index = lax.broadcasted_iota(jnp.int32, (BLOCK, BLOCK), 1)
    causal_mask = row_index >= col_index
    lower_tri = causal_mask.astype(jnp.float32)
    cumulative = jnp.einsum("hcs,ts->hct", blocks_decay, lower_tri, precision=HIGHEST)
    scores = jnp.einsum("ctn,csn->cts", blocks_c, blocks_b, preferred_element_type=jnp.float32)
    decay_diff = jnp.where(causal_mask, cumulative[..., :, None] - cumulative[..., None, :], 0.0)
    mix_weight = jnp.where(
        causal_mask, scores[None] * jnp.exp(decay_diff) * blocks_step[:, :, None, :], 0.0
    ).astype(jnp.bfloat16)
    intra_part = jnp.einsum(
        "hcts,cshp->cthp", mix_weight, blocks_x, preferred_element_type=jnp.float32
    )
    tail_weight = jnp.exp(cumulative[..., -1:] - cumulative) * blocks_step
    weighted_b = (blocks_b.astype(jnp.float32)[None] * tail_weight[..., None]).astype(jnp.bfloat16)
    updates = jnp.einsum(
        "cshp,hcsn->chpn", blocks_x, weighted_b, preferred_element_type=jnp.float32
    )
    totals = cumulative[..., -1]
    full_states = chain(totals[:, 0], updates[0], "ctx")[None]
    inter_part = (
        jnp.einsum("ctn,chpn->cthp", blocks_c.astype(jnp.float32), full_states, precision=HIGHEST)
        * jnp.exp(cumulative).transpose(1, 2, 0)[..., None]
    )
    output = (
        intra_part + inter_part + skip_gain[0][None, None, :, None] * blocks_x.astype(jnp.float32)
    )
    gated = output.reshape(token_count, local_width) * jax.nn.silu(
        gate_input[0].astype(jnp.float32)
    )
    squares = lax.psum(jnp.sum(gated * gated, axis=1), "mp")
    mean_square = squares / FEATURES
    normed = (gated * lax.rsqrt(mean_square + NORM_FLOOR)[:, None] * norm_gain[0][None]).astype(
        jnp.bfloat16
    )
    return project(normed, next_weight[0], gathered)[None]


def solution(mesh):
    return jax.shard_map(
        shards,
        mesh=mesh,
        in_specs=(
            P("section", "ctx", "mp"),
            P("section", "ctx", None),
            P("section", "ctx", "mp"),
            P("section", "mp", "ctx"),
            P("section", "mp"),
            P("section", "mp"),
            P("section", "mp"),
            P("section", None, "mp"),
            P("section", None, None),
            P("section", "mp"),
            P("section", "ctx", "mp"),
        ),
        out_specs=P("section", "ctx", "mp"),
        check_vma=False,
    )
```

```python
import functools

import jax
import jax.numpy as jnp
from jax import lax
from jax.experimental import pallas as pl
from jax.experimental.pallas import tpu as pltpu
from jax.sharding import PartitionSpec as P

STATE = 128
BLOCK = 256
FEATURES = 2048


NORM_FLOOR = 0.25
FEW = 8
HIGHEST = lax.Precision.HIGHEST


def from_behind(value, axis, steps):
    count = lax.axis_size(axis)
    first, last = (max(0, -steps), min(count, count - steps))
    return lax.ppermute(value, axis, [(source, source + steps) for source in range(first, last)])


def chain(total, update, axis):
    count = lax.axis_size(axis)
    place = lax.axis_index(axis)
    decay = jnp.exp(total)[:, None, None]
    state = jnp.zeros_like(update)

    def passed(state):
        return (decay * state + update).astype(jnp.bfloat16)

    if count > FEW:
        pairs = [(source, source + 1) for source in range(count - 1)]
        return lax.fori_loop(
            1,
            count,
            lambda _, state: lax.ppermute(passed(state), axis, pairs).astype(jnp.float32),
            state,
        )
    for step in range(1, count):
        came = lax.ppermute(passed(state), axis, [(step - 1, step)])
        state = jnp.where(place == step, came.astype(jnp.float32), state)
    return state


def gather_half(rows):
    count = lax.axis_size("ctx")
    half = count // 2
    blocks = []
    for step in range(1, half):
        pairs = [
            (base + (place + step) % half, base + place)
            for base in (0, half)
            for place in range(half)
        ]
        blocks.append(lax.ppermute(rows, "ctx", pairs))
    return jnp.concatenate(blocks, axis=0) if len(blocks) > 1 else blocks[0]


def project_kernel(
    sections,
    count,
    chunks,
    first,
    early,
    normed,
    weight,
    gathered_first,
    gathered_second,
    out,
    held,
    blocks,
    sends,
    recvs,
    weight_sem,
    route_send,
    route_recv,
    pass_send,
    pass_recv,
    part_send,
    part_recv,
    late_send,
    late_recv,
):
    section, place, core = (lax.axis_index(a) for a in ("section", "ctx", "mp"))
    half = count // 2
    side = place // half
    rows = normed.shape[0] // 2
    width = out.shape[1] // chunks
    depth = weight.shape[0]
    inner = lax.rem(place, half)

    def rows_of(owner):
        return pl.ds(pl.multiple_of(owner * depth, depth), depth)

    loads = [pltpu.make_async_copy(weight, held.at[rows_of(inner)], weight_sem.at[0])]
    for group, (gathered, low, high) in enumerate(
        ((gathered_first, 0, first), (gathered_second, first, early))
    ):
        for step in range(1, half):
            columns = pl.ds(low * width, (high - low) * width)
            loads.append(
                pltpu.make_async_copy(
                    gathered.at[pl.ds((step - 1) * depth, depth)],
                    held.at[rows_of(lax.rem(inner + step, half)), columns],
                    weight_sem.at[group * (half - 1) + step],
                )
            )
    for load in loads:
        load.start()

    def at(section, place, core):
        return {"section": section, "ctx": place, "mp": core}

    after = lax.rem(section + 1, sections)
    before = lax.rem(section + sections - 1, sections)
    mirror = lax.rem(place + half, count)
    target = lax.rem(place, half) + half * core
    peer = at(section, place, 1 - core)
    opposite = at(section, mirror, core)
    barrier = pltpu.get_barrier_semaphore()
    friends = [
        at(after, target, 0),
        at(after, target, 1),
        at(before, place, side),
        at(before, mirror, side),
        peer,
        opposite,
    ]
    siblings = [
        at(section, side * half + lax.rem(inner + step, half), core) for step in range(1, half)
    ]
    friends += siblings
    for friend in friends:
        pl.semaphore_signal(
            barrier, inc=1, device_id=friend, device_id_type=pl.DeviceIdType.MESH
        )
    pl.semaphore_wait(barrier, len(friends))

    slot = lax.rem(side + core, 2)
    routes = []
    for to in range(2):
        piece = pl.ds(to * rows, rows)
        routes.append(
            pltpu.make_async_remote_copy(
                src_ref=normed.at[piece],
                dst_ref=blocks.at[slot, piece],
                send_sem=route_send.at[to],
                recv_sem=route_recv.at[slot],
                device_id=at(after, target, to),
                device_id_type=pl.DeviceIdType.MESH,
            )
        )
        routes[-1].start()

    def late(step, index):
        columns = pl.ds(pl.multiple_of(index * width, width), width)
        return pltpu.make_async_remote_copy(
            src_ref=weight.at[:, columns],
            dst_ref=held.at[rows_of(inner), columns],
            send_sem=late_send.at[step - 1, index - early],
            recv_sem=late_recv.at[step - 1, index - early],
            device_id=siblings[step - 1],
            device_id_type=pl.DeviceIdType.MESH,
        )

    for index in range(early, chunks):
        for step in range(1, half):
            late(step, index).start()
    mine = pl.ds(pl.multiple_of(core * rows, rows), rows)
    passes = []
    for which in (1, 0):
        landed = blocks.at[which, mine]
        pltpu.make_async_copy(landed, landed, route_recv.at[which]).wait()
        passes.append(
            pltpu.make_async_remote_copy(
                src_ref=landed,
                dst_ref=landed,
                send_sem=pass_send.at[which],
                recv_sem=pass_recv.at[which],
                device_id=peer,
                device_id_type=pl.DeviceIdType.MESH,
            )
        )
        passes[-1].start()

    def part(index):
        return pltpu.make_async_remote_copy(
            src_ref=sends.at[index],
            dst_ref=recvs.at[index],
            send_sem=part_send.at[index],
            recv_sem=part_recv.at[index],
            device_id=opposite,
            device_id_type=pl.DeviceIdType.MESH,
        )

    def product(which, index):
        columns = pl.ds(pl.multiple_of(index * width, width), width)
        return jnp.dot(blocks[which], held[:, columns], preferred_element_type=jnp.float32)

    for load in loads:
        load.wait()
    passes[0].wait_recv()

    def give(index, carry):
        sends[index] = product(1, index).astype(sends.dtype)

        @pl.when(index > 0)
        def _():
            part(index - 1).start()

        return carry

    lax.fori_loop(0, early, give, 0)

    def give_late(index, carry):
        columns = pl.ds(pl.multiple_of(index * width, width), width)
        for step in range(1, half):
            source = lax.rem(inner + half - step, half)
            landed = held.at[rows_of(source), columns]
            pltpu.make_async_copy(landed, landed, late_recv.at[step - 1, index - early]).wait()
        return give(index, carry)

    lax.fori_loop(early, chunks, give_late, 0)
    passes[1].wait_recv()
    part(chunks - 1).start()

    def take(index, carry):
        own = product(0, index)
        part(index).wait_recv()
        columns = pl.ds(pl.multiple_of(index * width, width), width)
        out[:, columns] = (own + recvs[index].astype(jnp.float32)).astype(out.dtype)
        part(index).wait_send()
        return carry

    lax.fori_loop(0, chunks, take, 0)
    for copy in routes + passes:
        copy.wait_send()
    for index in range(early, chunks):
        for step in range(1, half):
            late(step, index).wait_send()


CHUNKS = 8
FIRST = 2
EARLY = 6


def project(normed, weight, gathered_first, gathered_second):
    sections, count = (lax.axis_size(a) for a in ("section", "ctx"))
    rows, depth = normed.shape
    width = weight.shape[1]
    half = count // 2
    chunks, first, early = CHUNKS, FIRST, EARLY
    piece = (chunks, rows, width // chunks)
    return pl.pallas_call(
        functools.partial(project_kernel, sections, count, chunks, first, early),
        out_shape=jax.ShapeDtypeStruct((rows, width), jnp.bfloat16),
        in_specs=[
            pl.BlockSpec(memory_space=pltpu.VMEM),
            pl.BlockSpec(memory_space=pl.ANY),
            pl.BlockSpec(memory_space=pl.ANY),
            pl.BlockSpec(memory_space=pl.ANY),
        ],
        out_specs=pl.BlockSpec(memory_space=pltpu.VMEM),
        scratch_shapes=[
            pltpu.VMEM((depth, width), jnp.bfloat16),
            pltpu.VMEM((2, rows, depth), jnp.bfloat16),
            pltpu.VMEM(piece, jnp.bfloat16),
            pltpu.VMEM(piece, jnp.bfloat16),
            pltpu.SemaphoreType.DMA((2 * half - 1,)),
            pltpu.SemaphoreType.DMA((2,)),
            pltpu.SemaphoreType.DMA((2,)),
            pltpu.SemaphoreType.DMA((2,)),
            pltpu.SemaphoreType.DMA((2,)),
            pltpu.SemaphoreType.DMA((chunks,)),
            pltpu.SemaphoreType.DMA((chunks,)),
            pltpu.SemaphoreType.DMA((half - 1, chunks - early)),
            pltpu.SemaphoreType.DMA((half - 1, chunks - early)),
        ],
        cost_estimate=pl.CostEstimate(
            flops=4 * rows * depth * width, bytes_accessed=2 * depth * width, transcendentals=0
        ),
        compiler_params=pltpu.CompilerParams(collective_id=0, has_side_effects=True),
        name="project",
    )(normed, weight, gathered_first, gathered_second)


def causal_conv(sequence, previous, weights):
    length = sequence.shape[0]
    padded = jnp.concatenate([previous, sequence], axis=0).astype(jnp.float32)
    summed = jnp.zeros(sequence.shape, jnp.float32)
    for offset in range(weights.shape[0]):
        summed = summed + weights[offset] * padded[offset : offset + length]
    return summed


def shards(
    head_input,
    state_proj,
    gate_input,
    step_raw,
    step_bias,
    decay_log,
    skip_gain,
    conv_head,
    conv_state,
    norm_gain,
    next_weight,
):
    tap_count = conv_head.shape[1]
    token_count = head_input.shape[1]
    local_width = head_input.shape[2]
    head_count = step_raw.shape[1]
    head_width = local_width // head_count
    block_count = token_count // BLOCK
    piece = next_weight.shape[2] // CHUNKS
    gathered_first = gather_half(next_weight[0, :, : piece * FIRST])
    gathered_second = gather_half(next_weight[0, :, piece * FIRST : piece * EARLY])
    tails = jnp.concatenate(
        [
            head_input[0, token_count - tap_count + 1 :],
            state_proj[0, token_count - tap_count + 1 :],
        ],
        axis=1,
    )
    previous = from_behind(tails, "ctx", 1)
    conv_x = jax.nn.silu(
        causal_conv(head_input[0], previous[:, :local_width], conv_head[0])
    ).astype(jnp.bfloat16)
    conv_bc = causal_conv(state_proj[0], previous[:, local_width:], conv_state[0]).astype(
        jnp.bfloat16
    )
    blocks_x = conv_x.reshape(block_count, BLOCK, head_count, head_width)
    blocks_b = conv_bc[:, :STATE].reshape(block_count, BLOCK, STATE)
    blocks_c = conv_bc[:, STATE:].reshape(block_count, BLOCK, STATE)
    step_size = jax.nn.softplus(step_raw[0] + step_bias[0][:, None])
    log_decay = -jnp.exp(decay_log[0])[:, None] * step_size
    blocks_step = step_size.reshape(head_count, block_count, BLOCK)
    blocks_decay = log_decay.reshape(head_count, block_count, BLOCK)
    row_index = lax.broadcasted_iota(jnp.int32, (BLOCK, BLOCK), 0)
    col_index = lax.broadcasted_iota(jnp.int32, (BLOCK, BLOCK), 1)
    causal_mask = row_index >= col_index
    lower_tri = causal_mask.astype(jnp.float32)
    cumulative = jnp.einsum("hcs,ts->hct", blocks_decay, lower_tri, precision=HIGHEST)
    scores = jnp.einsum("ctn,csn->cts", blocks_c, blocks_b, preferred_element_type=jnp.float32)
    decay_diff = jnp.where(causal_mask, cumulative[..., :, None] - cumulative[..., None, :], 0.0)
    mix_weight = jnp.where(
        causal_mask, scores[None] * jnp.exp(decay_diff) * blocks_step[:, :, None, :], 0.0
    ).astype(jnp.bfloat16)
    intra_part = jnp.einsum(
        "hcts,cshp->cthp", mix_weight, blocks_x, preferred_element_type=jnp.float32
    )
    tail_weight = jnp.exp(cumulative[..., -1:] - cumulative) * blocks_step
    weighted_b = (blocks_b.astype(jnp.float32)[None] * tail_weight[..., None]).astype(jnp.bfloat16)
    updates = jnp.einsum(
        "cshp,hcsn->chpn", blocks_x, weighted_b, preferred_element_type=jnp.float32
    )
    totals = cumulative[..., -1]
    update, gathered_first = lax.optimization_barrier((updates[0], gathered_first))
    full_states = chain(totals[:, 0], update, "ctx")[None]
    inter_part = (
        jnp.einsum("ctn,chpn->cthp", blocks_c.astype(jnp.float32), full_states, precision=HIGHEST)
        * jnp.exp(cumulative).transpose(1, 2, 0)[..., None]
    )
    output = (
        intra_part + inter_part + skip_gain[0][None, None, :, None] * blocks_x.astype(jnp.float32)
    )
    gated = output.reshape(token_count, local_width) * jax.nn.silu(
        gate_input[0].astype(jnp.float32)
    )
    squares = lax.psum(jnp.sum(gated * gated, axis=1), "mp")
    mean_square = squares / FEATURES
    normed = (gated * lax.rsqrt(mean_square + NORM_FLOOR)[:, None] * norm_gain[0][None]).astype(
        jnp.bfloat16
    )
    return project(normed, next_weight[0], gathered_first, gathered_second)[None]


def solution(mesh):
    return jax.shard_map(
        shards,
        mesh=mesh,
        in_specs=(
            P("section", "ctx", "mp"),
            P("section", "ctx", None),
            P("section", "ctx", "mp"),
            P("section", "mp", "ctx"),
            P("section", "mp"),
            P("section", "mp"),
            P("section", "mp"),
            P("section", None, "mp"),
            P("section", None, None),
            P("section", "mp"),
            P("section", "ctx", "mp"),
        ),
        out_specs=P("section", "ctx", "mp"),
        check_vma=False,
    )
```
